32 devices in a mesh: gx: 2 (over x), gy: 4 (over y, core), gz: 4 (over z).
Axes of the slice: x: 2, y: 2, z: 4, core: 2. Of those that a mesh axis runs over, the one named last changes fastest.
Arguments:
- charges: bfloat16 [8, 16, 16, 32, 128], P('gx', 'gy', 'gz'), may hold values from -6 to 6
- counts: int32 [8, 16, 16], P('gx', 'gy', 'gz'), may hold values from 32 to 128, as said below
- near_offsets: int32 [27, 3], replicated, may hold values from -1 to 1, as said below
- near_blocks: bfloat16 [27, 128, 128], replicated, may hold values from -0.109375 to 0.109375
- leaf_basis: bfloat16 [48, 128], replicated, may hold values from -0.5 to 0.5
- transfer: bfloat16 [8, 48, 48], replicated, may hold values from -0.625 to 0.625
- far_offsets: int32 [2, 32, 3], replicated, may hold values from -2 to 2, as said below
- coupling: bfloat16 [2, 32, 48, 48], replicated, may hold values from -0.15625 to 0.15625
- coarse_coupling: bfloat16 [2, 4, 4, 48, 48], replicated, may hold values from -0.3125 to 0.3125
Outputs:
- potentials: float32 [8, 16, 16, 32, 128], P('gx', 'gy', 'gz')
The draws below stay inside these ranges and needn't reach their ends.
Inputs may be any that keep to these rules, and one draw needn't show every extreme that they name: `counts`: in each device's block of 4 x 4 x 4 leaf boxes some box holds 128 points. `near_offsets`: each of the 27 offsets with components in -1, 0, 1 appears once. `far_offsets`: each level lists 32 distinct offsets whose largest component in magnitude is 2.
All inputs are finite; a program needn't handle non-finite values.
Results may differ from the reference program's by a relative error of at most 0.008.
Values may be sent and summed in bfloat16 or wider, within the bound.
A program may use at most 128 MiB of HBM per device.

```python
import jax
import jax.numpy as jnp
import numpy as np
from jax import lax

PTS = 128
RANK = 48
RHS = 32
STENCIL = 27
LIST = 32
BX = 4
BY = 4
BZ = 4
LX = 8
LY = 16
LZ = 16
CGX = 2
CGY = 4
CGZ = 4


def candidate_table():
    entries = []
    for first in range(-2, 3):
        for second in range(-2, 3):
            for third in range(-2, 3):
                if max(abs(first), abs(second), abs(third)) == 2:
                    entries.append([first, second, third])
    return np.array(entries, dtype=np.int32)


def draw_counts(key, part):
    base = jax.random.randint(jax.random.fold_in(key, 1), (LX, LY, LZ), PTS // 4, PTS + 1)
    chosen = jax.random.randint(jax.random.fold_in(key, 2), (LX // BX, LY // BY, LZ // BZ), 0, BX * BY * BZ)
    spread = jnp.repeat(jnp.repeat(jnp.repeat(chosen, BX, axis=0), BY, axis=1), BZ, axis=2)
    pos_x = (jnp.arange(LX, dtype=jnp.int32) % BX)[:, None, None]
    pos_y = (jnp.arange(LY, dtype=jnp.int32) % BY)[None, :, None]
    pos_z = (jnp.arange(LZ, dtype=jnp.int32) % BZ)[None, None, :]
    within = (pos_x * BY + pos_y) * BZ + pos_z
    return jnp.where(within == spread, PTS, base).astype(jnp.int32)


def draw_near_offsets(key, part):
    order = jax.random.permutation(jax.random.fold_in(key, 3), 27).astype(jnp.int32)
    return jnp.stack([order // 9 - 1, order // 3 % 3 - 1, order % 3 - 1], axis=1).astype(jnp.int32)


def draw_far_offsets(key, part):
    table = jnp.asarray(candidate_table())
    levels = []
    for level in range(2):
        picked = jax.random.permutation(jax.random.fold_in(key, 10 + level), table.shape[0])[:LIST]
        levels.append(table[picked])
    return jnp.stack(levels).astype(jnp.int32)


def block_levels(stream_key, extent, cuts, least, largest):
    factor_of, own = 1.0, jax.random.fold_in(stream_key, 6)
    for position, parts in cuts:
        draws = jnp.exp(jax.random.uniform(jax.random.fold_in(own, position), (parts,), jnp.float32, least / len(cuts), largest / len(cuts)))
        factor_of = factor_of * jnp.repeat(draws, extent[position] // parts).reshape([-1 if axis == position else 1 for axis in range(len(extent))])
    return factor_of


def centred(key, extent, deviation, limit, cuts=(), kind=jnp.bfloat16):
    values = jax.random.normal(key, extent, jnp.float32) * deviation
    if len(cuts) > 0:
        values = block_levels(key, extent, cuts, -0.22, 0.18) * values
    return jnp.clip(values, min=-limit, max=limit).astype(kind)


def setup_inputs(seed: int = 0) -> dict:
    arg_keys = jax.random.split(jax.random.key(seed), 10)
    charges = centred(arg_keys[0], (LX, LY, LZ, RHS, PTS), 1.0, 6.0, ((0, 2), (1, 4), (2, 4)))
    counts = draw_counts(jax.random.fold_in(arg_keys[9], 71), 0)
    near_offsets = draw_near_offsets(jax.random.fold_in(arg_keys[9], 71), 0)
    near_blocks = centred(arg_keys[3], (STENCIL, PTS, PTS), (STENCIL * PTS) ** -0.5, 0.109375)
    leaf_basis = centred(arg_keys[4], (RANK, PTS), PTS ** -0.5, 0.5)
    transfer = centred(arg_keys[5], (8, RANK, RANK), (2 * RANK) ** -0.5, 0.625)
    far_offsets = draw_far_offsets(jax.random.fold_in(arg_keys[9], 71), 0)
    coupling = centred(arg_keys[7], (2, LIST, RANK, RANK), (LIST * RANK) ** -0.5, 0.15625)
    coarse_coupling = centred(arg_keys[8], (CGX, CGY, CGZ, RANK, RANK), (CGX * CGY * CGZ * RANK // 4) ** -0.5, 0.3125)
    return {"charges": charges, "counts": counts, "near_offsets": near_offsets, "near_blocks": near_blocks, "leaf_basis": leaf_basis, "transfer": transfer, "far_offsets": far_offsets, "coupling": coupling, "coarse_coupling": coarse_coupling}


def shifted(field, offset):
    return jnp.roll(field, (-offset[0], -offset[1], -offset[2]), axis=(0, 1, 2))


def upward(moments, transfer):
    first_len, second_len, third_len, rank_count, columns = moments.shape
    split = moments.astype(jnp.float32).reshape(first_len // 2, 2, second_len // 2, 2, third_len // 2, 2, rank_count, columns)
    kids = split.transpose(0, 2, 4, 1, 3, 5, 6, 7).reshape(first_len // 2, second_len // 2, third_len // 2, 8, rank_count, columns)
    return jnp.einsum("ckj,xyzcjr->xyzkr", transfer.astype(jnp.float32), kids).astype(jnp.bfloat16)


def downward(parent, transfer):
    rounded = lax.optimization_barrier(parent.astype(jnp.bfloat16)).astype(jnp.float32)
    kids = jnp.einsum("cjk,xyzjr->xyzckr", transfer.astype(jnp.float32), rounded)
    first_len, second_len, third_len, rank_count, columns = parent.shape
    split = kids.reshape(first_len, second_len, third_len, 2, 2, 2, rank_count, columns)
    return split.transpose(0, 3, 1, 4, 2, 5, 6, 7).reshape(2 * first_len, 2 * second_len, 2 * third_len, rank_count, columns)


def couple_level(moments, offsets, matrices):
    wide = moments.astype(jnp.float32)
    mats = matrices.astype(jnp.float32)

    def step(total, index):
        moved = shifted(wide, offsets[index])
        return total + jnp.einsum("kj,xyzjr->xyzkr", mats[index], moved), None

    start = jnp.zeros(moments.shape, jnp.float32)
    total, unused = lax.scan(step, start, jnp.arange(offsets.shape[0], dtype=jnp.int32))
    return total


def coarse_level(moments, coarse_coupling):
    grid_x, grid_y, grid_z = moments.shape[:3]
    wide = moments.astype(jnp.float32)
    mats = coarse_coupling.astype(jnp.float32)

    def step(total, number):
        off_x = number // (grid_y * grid_z)
        off_y = (number // grid_z) % grid_y
        off_z = number % grid_z
        moved = jnp.roll(wide, (-off_x, -off_y, -off_z), axis=(0, 1, 2))
        return total + jnp.einsum("kj,xyzjr->xyzkr", mats[off_x, off_y, off_z], moved), None

    start = jnp.zeros(moments.shape, jnp.float32)
    total, unused = lax.scan(step, start, jnp.arange(grid_x * grid_y * grid_z, dtype=jnp.int32))
    return total


def reference(charges, counts, near_offsets, near_blocks, leaf_basis, transfer, far_offsets, coupling, coarse_coupling):
    capacity = charges.shape[4]
    live = (jnp.arange(capacity, dtype=jnp.int32) < counts[..., None]).astype(jnp.bfloat16)
    masked = charges * live[:, :, :, None, :]
    masked_wide = masked.astype(jnp.float32)
    blocks = near_blocks.astype(jnp.float32)

    def near_step(total, index):
        moved = shifted(masked_wide, near_offsets[index])
        return total + jnp.einsum("xyzrq,pq->xyzrp", moved, blocks[index]), None

    near, unused = lax.scan(near_step, jnp.zeros(charges.shape, jnp.float32), jnp.arange(near_offsets.shape[0], dtype=jnp.int32))
    basis = leaf_basis.astype(jnp.float32)
    moments_zero = jnp.einsum("kp,xyzrp->xyzkr", basis, masked_wide).astype(jnp.bfloat16)
    moments_one = upward(moments_zero, transfer)
    moments_two = upward(moments_one, transfer)
    local_zero = couple_level(moments_zero, far_offsets[0], coupling[0])
    local_one = couple_level(moments_one, far_offsets[1], coupling[1])
    local_two = coarse_level(moments_two, coarse_coupling)
    total_one = local_one + downward(local_two, transfer)
    total_zero = local_zero + downward(total_one, transfer)
    rounded = lax.optimization_barrier(total_zero.astype(jnp.bfloat16)).astype(jnp.float32)
    far = jnp.einsum("kp,xyzkr->xyzrp", basis, rounded)
    return (near + far) * live[:, :, :, None, :].astype(jnp.float32)
```

```python
import functools

import jax
import jax.numpy as jnp
from jax import lax
from jax.experimental import pallas as pl
from jax.experimental.pallas import tpu as pltpu
from jax.sharding import PartitionSpec as P

MESH = pl.DeviceIdType.MESH
AXES = ("gx", "gy", "gz")
F32 = jnp.float32
BF16 = jnp.bfloat16
NT = (((1,), (1,)), ((), ()))
NN = (((1,), (0,)), ((), ()))


def dot(a, b, dims):
    return lax.dot_general(a, b, dims, preferred_element_type=F32)


def kernel(
    sizes,
    near_offsets,
    counts,
    far_offsets,
    charges_hbm,
    basis,
    transfer,
    near_hbm,
    coupling_hbm,
    coarse_hbm,
    out,
    charges,
    ext,
    mom,
    one,
    two,
    near_w,
    coupling_raw,
    coarse_raw,
    far_w,
    coarse_w,
    trans_w,
    basis_w,
    near_acc,
    far_acc,
    one_acc,
    inverse,
    local_sem,
    send_sem,
    recv_sem,
    gsend,
    grecv,
):
    bx, by, bz, rhs, pts = charges.shape
    rank = basis.shape[0]
    half = rhs // 2
    lane = pts // 2
    me = [lax.axis_index(a) for a in AXES]
    steps = coupling_raw.shape[1]
    cells = sizes[0] * sizes[1] * sizes[2]
    hx, hy, hz = bx // 2, by // 2, bz // 2

    charges_copy = pltpu.make_async_copy(charges_hbm, charges, local_sem.at[3])
    near_copy = pltpu.make_async_copy(near_hbm, near_w, local_sem.at[0])
    coupling_copy = pltpu.make_async_copy(coupling_hbm, coupling_raw, local_sem.at[1])
    coarse_copy = pltpu.make_async_copy(coarse_hbm, coarse_raw, local_sem.at[2])
    charges_copy.start()
    near_copy.start()
    coupling_copy.start()
    coarse_copy.start()

    barrier = pltpu.get_barrier_semaphore()
    peers = 0
    for axis in range(3):
        for d in range(1, sizes[axis]):
            other = lax.rem(me[axis] + d, sizes[axis])
            pl.semaphore_signal(barrier, inc=1, device_id={AXES[axis]: other}, device_id_type=MESH)
            peers += 1

    slots = [0]

    def halo(ref, own, width, order):
        high = [ref.shape[d] == own[d] + 2 * width for d in range(3)]
        sides = ["lh" if high[d] else "l" for d in range(3)]
        part = {
            "o": lambda d: pl.ds(width, own[d]),
            "l": lambda d: pl.ds(0, width),
            "h": lambda d: pl.ds(width + own[d], width),
        }
        first, second, third = order

        def moves(axis, fixed):
            def view(start):
                index = [part[fixed.get(d, "o")](d) for d in range(3)]
                index[axis] = pl.ds(start, width)
                return ref.at[tuple(index)]

            n = own[axis]
            pairs = [(n, 0, 1)]
            if high[axis]:
                pairs.append((width, width + n, sizes[axis] - 1))
            copies = []
            for src, dst, shift in pairs:
                slot = slots[0]
                slots[0] += 1
                copies.append(
                    pltpu.make_async_remote_copy(
                        src_ref=view(src),
                        dst_ref=view(dst),
                        send_sem=send_sem.at[slot],
                        recv_sem=recv_sem.at[slot],
                        device_id={AXES[axis]: lax.rem(me[axis] + shift, sizes[axis])},
                        device_id_type=MESH,
                    )
                )
            return copies

        groups = {"A": moves(first, {}), "B": moves(second, {}), "C": moves(third, {})}
        groups["AB"] = [moves(second, {first: a}) for a in sides[first]]
        groups["AC"] = [moves(third, {first: a}) for a in sides[first]]
        groups["BC"] = [moves(third, {second: b}) for b in sides[second]]
        groups["ABC"] = [
            [moves(third, {first: a, second: b}) for b in sides[second]] for a in sides[first]
        ]
        return groups

    def flat(items):
        if isinstance(items, (list, tuple)):
            return [c for item in items for c in flat(item)]
        return [items]

    def start(items):
        for c in flat(items):
            c.start()

    def arrive(items):
        for c in flat(items):
            c.wait_recv()

    def got_first(groups):
        for k, copy in enumerate(groups["A"]):
            copy.wait_recv()
            start(groups["AB"][k])
            start(groups["AC"][k])

    def got_second(groups):
        for k, copy in enumerate(groups["B"]):
            copy.wait_recv()
            start(groups["BC"][k])

    def got_edge(groups):
        for a, copies in enumerate(groups["AB"]):
            for b, copy in enumerate(copies):
                copy.wait_recv()
                start(groups["ABC"][a][b])

    ring = (2, 0, 1)

    def gather(stage):
        axis = ring[stage]
        done = ring[:stage]
        base = sum(sizes[d] - 1 for d in done)

        def view(place):
            index = [pl.ds(0, sizes[d]) if d in done else pl.ds(me[d], 1) for d in range(3)]
            index[axis] = pl.ds(place, 1)
            return two.at[tuple(index)]

        sends, receives = [], []
        for d in range(1, sizes[axis]):
            for place, other, copies in (
                (me[axis], lax.rem(me[axis] + d, sizes[axis]), sends),
                (lax.rem(me[axis] + sizes[axis] - d, sizes[axis]), None, receives),
            ):
                copies.append(
                    pltpu.make_async_remote_copy(
                        src_ref=view(place),
                        dst_ref=view(place),
                        send_sem=gsend.at[base + d - 1],
                        recv_sem=grecv.at[base + d - 1],
                        device_id={AXES[axis]: place if other is None else other},
                        device_id_type=MESH,
                    )
                )
        return sends, receives

    ch = halo(ext, (bx, by, bz), 1, (0, 2, 1))
    mo = halo(mom, (bx, by, bz), 2, (2, 0, 1))
    on = halo(one, (hx, hy, hz), 2, (0, 2, 1))
    tw = [gather(k) for k in range(3)]

    basis_w[...] = jnp.zeros(basis_w.shape, BF16)
    basis_w[0:rank, 0:pts] = basis[...]
    basis_w[lane : lane + rank, pts : 2 * pts] = basis[...]
    trans_w[...] = jnp.zeros(trans_w.shape, BF16)
    for c in range(8):
        trans_w[c, 0:rank, 0:rank] = transfer[c]
        trans_w[c, lane : lane + rank, lane : lane + rank] = transfer[c]
    far_w[...] = jnp.zeros(far_w.shape, BF16)

    lanes = lax.broadcasted_iota(jnp.int32, (half, pts), 1)
    charges_copy.wait()

    def mask_row(b, carry):
        x, y = b // by, b % by
        for z in range(bz):
            live = (lanes < counts[x, y, z]).astype(F32).astype(BF16)
            live = jnp.concatenate([live, live], axis=0)
            ext[1 + x, 1 + y, 1 + z] = charges[x, y, z] * live
        return carry

    lax.fori_loop(0, bx * by, mask_row, 0)
    pl.semaphore_wait(barrier, peers)
    start(ch["A"])
    start(ch["C"])

    def moments(x, carry):
        low = ext[1 + x, 1 : 1 + by, 1 : 1 + bz, 0:half].reshape(by * bz * half, pts)
        high = ext[1 + x, 1 : 1 + by, 1 : 1 + bz, half:rhs].reshape(by * bz * half, pts)
        value = dot(jnp.concatenate([low, high], axis=1), basis_w[...], NT).astype(BF16)
        mom[2 + x, 2 : 2 + by, 2 : 2 + bz] = value.reshape(by, bz, half, pts)
        return carry

    lax.fori_loop(0, bx, moments, 0)
    start(mo["A"])
    start(mo["C"])

    parents = [(a, b, c) for a in range(hx) for b in range(hy) for c in range(hz)]
    kids = [(i, j, l) for i in range(2) for j in range(2) for l in range(2)]
    total = jnp.zeros((len(parents) * half, pts), F32)
    for number, (i, j, l) in enumerate(kids):
        rows = jnp.concatenate(
            [mom[2 + 2 * a + i, 2 + 2 * b + j, 2 + 2 * c + l] for a, b, c in parents], axis=0
        )
        total = total + dot(rows, trans_w[number], NT)
    value = total.astype(BF16)
    for n, (a, b, c) in enumerate(parents):
        one[2 + a, 2 + b, 2 + c] = value[n * half : (n + 1) * half]
    start(on["A"])
    start(mo["B"])
    start(on["B"])
    start(on["C"])
    total = jnp.zeros((half, pts), F32)
    for number in range(8):
        total = total + dot(value[number * half : (number + 1) * half], trans_w[number], NT)
    two[me[0], me[1], me[2]] = total.astype(BF16)
    start(tw[0][0])
    start(ch["B"])

    stencil = near_offsets.shape[1]
    codes = []
    for number in range(stencil):
        x, y, z = (near_offsets[d, number] + 1 for d in range(3))
        codes.append(x * 9 + y * 3 + z)

    def invert(c, carry):
        found = jnp.int32(0)
        for number in range(stencil):
            found = found + jnp.where(codes[number] == c, number, 0)
        inverse[c] = jnp.minimum(found, stencil - 1)
        return carry

    lax.fori_loop(0, stencil, invert, 0)
    coupling_copy.wait()

    def build_far(t, carry):
        for level in range(2):
            for k in range(4):
                value = coupling_raw[level, 4 * t + k]
                for s in range(2):
                    col = k * pts + s * lane
                    far_w[level, t, s * lane : s * lane + rank, col : col + rank] = value
        return carry

    lax.fori_loop(0, steps // 4, build_far, 0)
    near_copy.wait()

    blank = jnp.zeros((pts, pts), BF16)

    def near_rows(dx, dz):
        columns = []
        for k in range(4):
            planes = [
                ext[pl.ds(1 + dx, bx), 2 * j + k, pl.ds(1 + dz, bz)].reshape(bx * bz * rhs, pts)
                for j in range(by // 2)
            ]
            columns.append(jnp.concatenate(planes, axis=0))
        return columns

    def near_weights(dx, dz):
        blocks = [near_w[inverse[(dx + 1) * 9 + k * 3 + dz + 1]] for k in range(3)]
        return blocks + [blank], [blank] + blocks

    def near_product(places):
        rows, even, odd = [], [], []
        for dx, dz in places:
            rows += near_rows(dx, dz)
            first, second = near_weights(dx, dz)
            even += first
            odd += second
        mats = jnp.concatenate(
            [jnp.concatenate(even, axis=1), jnp.concatenate(odd, axis=1)], axis=0
        )
        return dot(jnp.concatenate(rows, axis=1), mats, NT)

    arrive(ch["C"])
    near_acc[...] = near_product([(0, 0)])

    got_first(ch)
    got_first(on)
    got_first(mo)
    arrive(tw[0][1])
    start(tw[1][0])

    coarse_w[...] = jnp.zeros(coarse_w.shape, BF16)
    coarse_copy.wait()

    def build_coarse(t, carry):
        for k in range(2):
            r = 2 * t + k
            x, y, z = r // (sizes[1] * sizes[2]), r // sizes[2] % sizes[1], r % sizes[2]
            value = coarse_raw[x, y, z]
            for s in range(2):
                col = k * pts + s * lane
                coarse_w[t, s * lane : s * lane + rank, col : col + rank] = value
        return carry

    lax.fori_loop(0, cells // 2, build_coarse, 0)

    got_second(on)
    arrive(ch["AC"])
    near_acc[...] += near_product([(-1, 0), (1, 0)])
    arrive(tw[1][1])
    start(tw[2][0])
    got_second(mo)
    got_edge(on)
    got_second(ch)
    got_edge(mo)
    got_edge(ch)
    arrive(tw[2][1])

    group = 16

    def coarse_step(u, total):
        rows, mats = [], []
        for k in range(group):
            t = u * group + k
            for r in (2 * t, 2 * t + 1):
                x, y, z = r // (sizes[1] * sizes[2]), r // sizes[2] % sizes[1], r % sizes[2]
                rows.append(
                    two[
                        lax.rem(me[0] + x, sizes[0]),
                        lax.rem(me[1] + y, sizes[1]),
                        lax.rem(me[2] + z, sizes[2]),
                    ]
                )
            mats.append(coarse_w[t])
        return total + dot(jnp.concatenate(rows, axis=1), jnp.concatenate(mats, axis=1), NT)

    local_two = lax.fori_loop(
        0, cells // 2 // group, coarse_step, jnp.zeros((half, pts), F32)
    )

    arrive([on["C"], on["AC"], on["BC"], on["ABC"]])

    def far_window(ref, level, e, count):
        ox, oy, oz = (far_offsets[d, level, e] + 2 for d in range(3))
        planes = []
        for i in range(count[0]):
            x = lax.rem(ox + i, ref.shape[0])
            v = ref[x, pl.ds(oy, count[1]), pl.ds(oz, count[2])]
            planes.append(v.reshape(count[1] * count[2] * half, pts))
        return jnp.concatenate(planes, axis=0)

    def far_product(ref, level, t, many, count):
        rows = [far_window(ref, level, 4 * t + k, count) for k in range(4 * many)]
        mats = [far_w[level, t + k] for k in range(many)]
        return dot(jnp.concatenate(rows, axis=1), jnp.concatenate(mats, axis=1), NT)

    one_acc[...] = jnp.zeros(one_acc.shape, F32)

    def far_one(t, carry):
        one_acc[...] += far_product(one, 1, 4 * t, 4, (hx, hy, hz))
        return carry

    lax.fori_loop(0, steps // 16, far_one, 0)

    rounded = local_two.astype(BF16)
    for number in range(8):
        rows = slice(number * half, (number + 1) * half)
        one_acc[rows, :] += dot(rounded, trans_w[number], NN)

    rounded = one_acc[...].astype(BF16)
    for number, (i, j, l) in enumerate(kids):
        value = dot(rounded, trans_w[number], NN)
        for n, (a, b, c) in enumerate(parents):
            box = ((2 * a + i) * by + 2 * b + j) * bz + 2 * c + l
            far_acc[box * half : (box + 1) * half, :] = value[n * half : (n + 1) * half]

    arrive(ch["BC"])
    near_acc[...] += near_product([(0, -1), (0, 1)])

    arrive([mo["C"], mo["AC"], mo["BC"], mo["ABC"]])

    def far_zero(t, carry):
        far_acc[...] += far_product(mom, 0, 2 * t, 2, (bx, by, bz))
        return carry

    lax.fori_loop(0, steps // 8, far_zero, 0)

    arrive(ch["ABC"])

    def near_corner(t, carry):
        near_acc[...] += near_product([(2 * t - 1, -1), (2 * t - 1, 1)])
        return carry

    lax.fori_loop(0, 2, near_corner, 0)

    def finish(x, carry):
        span = by * bz * half
        rows = far_acc[pl.ds(pl.multiple_of(x * span, span), span), :].astype(BF16)
        value = dot(rows, basis_w[...], NN)
        for b in range(by * bz):
            y, z = b // bz, b % bz
            live = (lanes < counts[x, y, z]).astype(F32)
            live = jnp.concatenate([live, live], axis=0)
            far = jnp.concatenate(
                [
                    value[b * half : (b + 1) * half, 0:pts],
                    value[b * half : (b + 1) * half, pts : 2 * pts],
                ],
                axis=0,
            )
            at = pl.multiple_of(((y // 2 * bx + x) * bz + z) * rhs, rhs)
            col = y % 2 * pts
            out[x, y, z] = (near_acc[pl.ds(at, rhs), col : col + pts] + far) * live
        return carry

    lax.fori_loop(0, bx, finish, 0)

    for groups in (ch, mo, on):
        for c in flat(list(groups.values())):
            c.wait_send()
    for sends, receives in tw:
        for c in sends:
            c.wait_send()


def body(
    sizes,
    charges,
    counts,
    near_offsets,
    near_blocks,
    leaf_basis,
    transfer,
    far_offsets,
    coupling,
    coarse_coupling,
):
    bx, by, bz, rhs, pts = charges.shape
    half = rhs // 2
    stencil = near_offsets.shape[0]
    boxes = bx * by * bz
    hx, hy, hz = bx // 2, by // 2, bz // 2
    one_x = hx + 2 if sizes[0] * hx == hx + 2 else hx + 4
    levels, steps = coupling.shape[:2]
    cells = sizes[0] * sizes[1] * sizes[2]
    peers = sum(sizes) - 3
    smem = pl.BlockSpec(memory_space=pltpu.SMEM)
    vmem = pl.BlockSpec(memory_space=pltpu.VMEM)
    hbm = pl.BlockSpec(memory_space=pl.ANY)
    return pl.pallas_call(
        functools.partial(kernel, sizes),
        out_shape=pltpu.VMEM(charges.shape, F32),
        in_specs=[smem, smem, smem, hbm, vmem, vmem, hbm, hbm, hbm],
        out_specs=vmem,
        scratch_shapes=[
            pltpu.VMEM(charges.shape, BF16),
            pltpu.VMEM((bx + 2, by + 2, bz + 2, rhs, pts), BF16),
            pltpu.VMEM((bx + 4, by + 4, bz + 4, half, pts), BF16),
            pltpu.VMEM((one_x, hy + 4, hz + 4, half, pts), BF16),
            pltpu.VMEM(tuple(sizes) + (half, pts), BF16),
            pltpu.VMEM(near_blocks.shape, BF16),
            pltpu.VMEM(coupling.shape, BF16),
            pltpu.VMEM(coarse_coupling.shape, BF16),
            pltpu.VMEM((levels, steps // 4, pts, 4 * pts), BF16),
            pltpu.VMEM((cells // 2, pts, 2 * pts), BF16),
            pltpu.VMEM((8, pts, pts), BF16),
            pltpu.VMEM((pts, 2 * pts), BF16),
            pltpu.VMEM((boxes // 2 * rhs, 2 * pts), F32),
            pltpu.VMEM((boxes * half, pts), F32),
            pltpu.VMEM((hx * hy * hz * half, pts), F32),
            pltpu.SMEM((stencil,), jnp.int32),
            pltpu.SemaphoreType.DMA((4,)),
            pltpu.SemaphoreType.DMA((78,)),
            pltpu.SemaphoreType.DMA((78,)),
            pltpu.SemaphoreType.DMA((peers,)),
            pltpu.SemaphoreType.DMA((peers,)),
        ],
        compiler_params=pltpu.CompilerParams(
            collective_id=0, has_side_effects=True, vmem_limit_bytes=56 * 1024 * 1024
        ),
    )(
        near_offsets.T,
        counts,
        far_offsets.transpose(2, 0, 1),
        charges,
        leaf_basis,
        transfer,
        near_blocks,
        coupling,
        coarse_coupling,
    )


def solution(mesh):
    sizes = tuple(mesh.shape[a] for a in AXES)
    in_specs = (
        P("gx", "gy", "gz", None, None),
        P("gx", "gy", "gz"),
        P(),
        P(),
        P(),
        P(),
        P(),
        P(),
        P(),
    )
    out_specs = P("gx", "gy", "gz", None, None)
    return jax.shard_map(
        functools.partial(body, sizes),
        mesh=mesh,
        in_specs=in_specs,
        out_specs=out_specs,
        check_vma=False,
    )
```

```python
import functools

import jax
import jax.numpy as jnp
from jax import lax
from jax.experimental import pallas as pl
from jax.experimental.pallas import tpu as pltpu
from jax.sharding import PartitionSpec as P

MESH = pl.DeviceIdType.MESH
AXES = ("gx", "gy", "gz")
F32 = jnp.float32
BF16 = jnp.bfloat16
NT = (((1,), (1,)), ((), ()))
NN = (((1,), (0,)), ((), ()))


def dot(a, b, dims):
    return lax.dot_general(a, b, dims, preferred_element_type=F32)


def kernel(
    sizes,
    near_offsets_hbm,
    counts_hbm,
    far_offsets_hbm,
    charges_hbm,
    basis_hbm,
    transfer_hbm,
    near_hbm,
    coupling_hbm,
    coarse_hbm,
    out,
    near_offsets,
    counts,
    far_offsets,
    charges,
    basis,
    transfer,
    ext,
    mom,
    one,
    two,
    near_w,
    coupling_raw,
    coarse_raw,
    far_w,
    coarse_w,
    trans_w,
    basis_w,
    spread,
    near_acc,
    far_acc,
    one_acc,
    span,
    inverse,
    local_sem,
    send_sem,
    recv_sem,
):
    bx, by, bz, rhs, pts = charges.shape
    rank = basis.shape[0]
    half = rhs // 2
    lane = pts // 2
    me = [lax.axis_index(a) for a in AXES]
    steps = coupling_raw.shape[1]
    cells = sizes[0] * sizes[1] * sizes[2]
    hx, hy, hz = bx // 2, by // 2, bz // 2

    pairs = (
        (counts_hbm, counts),
        (charges_hbm, charges),
        (basis_hbm, basis),
        (transfer_hbm, transfer),
        (near_offsets_hbm, near_offsets),
        (far_offsets_hbm, far_offsets),
        (near_hbm, near_w),
        (coupling_hbm, coupling_raw),
        (coarse_hbm, coarse_raw),
    )
    local = [
        pltpu.make_async_copy(src, dst, local_sem.at[n]) for n, (src, dst) in enumerate(pairs)
    ]
    for copy in local:
        copy.start()

    barrier = pltpu.get_barrier_semaphore()
    peers = 0
    for axis in range(3):
        for d in range(1, sizes[axis]):
            other = lax.rem(me[axis] + d, sizes[axis])
            pl.semaphore_signal(barrier, inc=1, device_id={AXES[axis]: other}, device_id_type=MESH)
            peers += 1

    slots = [0]
    sent = [0]

    def tiles_of(ref):
        count = 1
        for n in ref.shape:
            count *= n
        return count // (half * pts)

    class Batch:
        def __init__(self):
            self.sem = recv_sem.at[slots[0]]
            slots[0] += 1
            self.copies = []
            self.tiles = 0

        def add(self, src, dst, device):
            self.copies.append(
                pltpu.make_async_remote_copy(
                    src_ref=src,
                    dst_ref=dst,
                    send_sem=send_sem.at[0],
                    recv_sem=self.sem,
                    device_id=device,
                    device_id_type=MESH,
                )
            )
            self.tiles += tiles_of(dst)

        def start(self, only=None):
            for c in self.copies if only is None else self.copies[only]:
                c.start()
            if only is None:
                sent[0] += self.tiles

        def wait(self):
            drain(self.sem, self.tiles)

    def drain(sem, tiles):
        while tiles > 0:
            n = min(tiles, span.shape[0])
            view = span.at[pl.ds(0, n)]
            pltpu.make_async_copy(view, view, sem).wait()
            tiles -= n

    def halo(ref, own, width, order, packed):
        extent = [ref.shape[d] for d in ((0, 2, 4) if packed else (0, 1, 2))]
        high = [extent[d] == own[d] + 2 * width[d] for d in range(3)]
        sides = ["lh" if high[d] else "l" for d in range(3)]
        part = {
            "o": lambda d: pl.ds(width[d], own[d]),
            "l": lambda d: pl.ds(0, width[d]),
            "h": lambda d: pl.ds(width[d] + own[d], width[d]),
        }
        first, second, third = order

        def moves(batch, axis, fixed, only="lh"):
            def views(start):
                index = [part[fixed.get(d, "o")](d) for d in range(3)]
                index[axis] = pl.ds(start, w)
                if not packed:
                    return [ref.at[tuple(index)]]
                return [
                    ref.at[index[0], i, index[1], pl.ds(0, 2 - i), index[2]] for i in range(2)
                ]

            n, w = own[axis], width[axis]
            if "l" in only:
                target = {AXES[axis]: lax.rem(me[axis] + 1, sizes[axis])}
                for src, dst in zip(views(n), views(0)):
                    batch.add(src, dst, target)
            if "h" in only and high[axis]:
                target = {AXES[axis]: lax.rem(me[axis] + sizes[axis] - 1, sizes[axis])}
                for src, dst in zip(views(w), views(w + n)):
                    batch.add(src, dst, target)
            return batch

        groups = {"A": [moves(Batch(), first, {}, side) for side in sides[first]]}
        groups["B"] = moves(Batch(), second, {})
        groups["AB"] = Batch()
        for a in sides[first]:
            moves(groups["AB"], second, {first: a})
        last = [Batch() for k in range(1 if packed else 4)]
        cuts = []
        for k, places in enumerate(
            (
                [{}],
                [{first: a} for a in sides[first]],
                [{second: b} for b in sides[second]],
                [{first: a, second: b} for a in sides[first] for b in sides[second]],
            )
        ):
            batch = last[0] if packed else last[k]
            begin = len(batch.copies)
            for fixed in places:
                moves(batch, third, fixed)
            cuts.append((batch, begin, len(batch.copies)))
        groups["last"] = last
        for batch in last:
            sent[0] += batch.tiles

        def send(k, low=0, high=None):
            batch, begin, end = cuts[k]
            n = end - begin
            high = n if high is None else high
            batch.start(slice(begin + low, begin + high))

        groups["send"] = send
        groups["per"] = len(cuts[0][0].copies[: cuts[0][2]])
        return groups

    def got_first(groups):
        per_second = len(groups["B"].copies)
        per_third = groups["per"]
        for k, batch in enumerate(groups["A"]):
            batch.wait()
            groups["AB"].start(slice(k * per_second, (k + 1) * per_second))
            groups["send"](1, k * per_third, (k + 1) * per_third)
        sent[0] += groups["AB"].tiles

    def got_second(groups):
        groups["B"].wait()
        groups["send"](2)

    def got_edge(groups):
        groups["AB"].wait()
        groups["send"](3)

    ring = (2, 1, 0)

    def gather(stage):
        axis = ring[stage]
        done = ring[:stage]
        batch = Batch()

        index = [pl.ds(0, sizes[d]) if d in done else pl.ds(me[d], 1) for d in range(3)]
        view = two.at[tuple(index)]
        for d in range(1, sizes[axis]):
            batch.add(view, view, {AXES[axis]: lax.rem(me[axis] + d, sizes[axis])})
        return batch

    parts = spread.shape[1] // pts
    third = rank // parts
    ch = halo(ext, (bx, by, bz), (1, 1, 1), (0, 2, 1), False)
    mo = halo(mom, (hx, hy, bz), (1, 1, 2), (2, 0, 1), True)
    on = halo(one, (hx // 2, hy // 2, hz), (1, 1, 2), (0, 2, 1), True)
    tw = [gather(k) for k in range(3)]

    local[2].wait()
    local[3].wait()
    basis_w[...] = jnp.zeros(basis_w.shape, BF16)
    basis_w[0:rank, 0:pts] = basis[...]
    basis_w[lane : lane + rank, pts : 2 * pts] = basis[...]
    trans_w[...] = jnp.zeros(trans_w.shape, BF16)
    for c in range(8):
        trans_w[c, 0:rank, 0:rank] = transfer[c]
        trans_w[c, lane : lane + rank, lane : lane + rank] = transfer[c]
    far_w[...] = jnp.zeros(far_w.shape, BF16)
    target = lax.broadcasted_iota(jnp.int32, (pts, pts), 0)
    source = lax.broadcasted_iota(jnp.int32, (pts, pts), 1)
    moved = jnp.where(source % lane >= rank, source - rank, -pts)
    for q in range(parts):
        hit = (target == moved + q * third).astype(F32).astype(BF16)
        spread[:, q * pts : (q + 1) * pts] = hit

    def pack(last):
        return dot(last, spread[...], NN).astype(BF16)

    def unpack(tiles):
        return dot(jnp.concatenate(tiles, axis=1), spread[...], NT).astype(BF16)

    lanes = lax.broadcasted_iota(jnp.int32, (half, pts), 1)
    local[0].wait()
    local[1].wait()

    def mask_row(b, carry):
        x, y = b // by, b % by
        for z in range(bz):
            live = (lanes < counts[x, y, z]).astype(F32).astype(BF16)
            live = jnp.concatenate([live, live], axis=0)
            ext[1 + x, 1 + y, 1 + z] = charges[x, y, z] * live
        return carry

    lax.fori_loop(0, bx * by, mask_row, 0)
    pl.semaphore_wait(barrier, peers)
    for batch in ch["A"]:
        batch.start()
    ch["send"](0)

    values = []
    for x in range(bx):
        low = ext[1 + x, 1 : 1 + by, 1 : 1 + bz, 0:half].reshape(by * bz * half, pts)
        high = ext[1 + x, 1 : 1 + by, 1 : 1 + bz, half:rhs].reshape(by * bz * half, pts)
        value = dot(jnp.concatenate([low, high], axis=1), basis_w[...], NT).astype(BF16)
        values.append(value.reshape(hy, 2, bz * half, pts))
    for a in range(hx):
        for b in range(hy):
            tiles = [values[2 * a + q // 2][b, q % 2] for q in range(parts + 1)]
            extra = pack(tiles[parts])
            for q in range(parts + 1):
                tile = tiles[q]
                if q < parts:
                    tile = tile + extra[:, q * pts : (q + 1) * pts]
                mom[1 + a, q // 2, 1 + b, q % 2, 2 : 2 + bz] = tile.reshape(bz, half, pts)
    for batch in mo["A"]:
        batch.start()
    mo["send"](0)
    mo["B"].start()
    ch["B"].start()

    parents = [(a, b, c) for a in range(hx) for b in range(hy) for c in range(hz)]
    kids = [(i, j, l) for i in range(2) for j in range(2) for l in range(2)]
    total = jnp.zeros((len(parents) * half, pts), F32)
    for number, (i, j, l) in enumerate(kids):
        rows = jnp.concatenate(
            [mom[1 + a, i, 1 + b, j, 2 + 2 * c + l] for a, b, c in parents], axis=0
        )
        total = total + dot(rows, trans_w[number], NT)
    value = total.astype(BF16)
    pieces = {p: value[n * half : (n + 1) * half] for n, p in enumerate(parents)}
    for a in range(hx // 2):
        for b in range(hy // 2):
            tiles = [
                jnp.concatenate([pieces[2 * a + i, 2 * b + j, c] for c in range(hz)], axis=0)
                for i in range(2)
                for j in range(2)
            ]
            extra = pack(tiles[parts])
            for q in range(parts + 1):
                tile = tiles[q]
                if q < parts:
                    tile = tile + extra[:, q * pts : (q + 1) * pts]
                one[1 + a, q // 2, 1 + b, q % 2, 2 : 2 + hz] = tile.reshape(hz, half, pts)
    total = jnp.zeros((half, pts), F32)
    for number in range(8):
        total = total + dot(value[number * half : (number + 1) * half], trans_w[number], NT)
    two[me[0], me[1], me[2]] = total.astype(BF16)
    for batch in on["A"]:
        batch.start()
    tw[0].start()
    on["B"].start()
    on["send"](0)

    local[4].wait()
    local[5].wait()
    stencil = near_offsets.shape[1]
    words = [jnp.int32(0)] * 9
    for number in range(stencil):
        x, y, z = (near_offsets[d, number] + 1 for d in range(3))
        key = x * 3 + y
        value = jnp.where(z == 0, number, jnp.where(z == 1, number * 32, number * 1024))
        words = [w + jnp.where(key == k, value, 0) for k, w in enumerate(words)]
    for k in range(9):
        inverse[k] = words[k]
    local[7].wait()

    def build_far(t, carry):
        for level in range(2):
            for u in range(2):
                for k in range(4):
                    value = coupling_raw[level, 8 * t + 4 * u + k]
                    for s in range(2):
                        col = k * pts + s * lane
                        far_w[level, 2 * t + u, s * lane : s * lane + rank, col : col + rank] = value
        return carry

    lax.fori_loop(0, steps // 8, build_far, 0)
    local[6].wait()

    blank = jnp.zeros((pts, pts), BF16)

    def near_rows(dx, dz):
        columns = []
        for k in range(4):
            planes = [
                ext[pl.ds(1 + dx, bx), 2 * j + k, pl.ds(1 + dz, bz)].reshape(bx * bz * rhs, pts)
                for j in range(by // 2)
            ]
            columns.append(jnp.concatenate(planes, axis=0))
        return columns

    def near_weights(dx, dz):
        blocks = []
        for k in range(3):
            found = (inverse[(dx + 1) * 3 + k] // 32 ** (dz + 1)) % 32
            blocks.append(near_w[jnp.minimum(found, near_w.shape[0] - 1)])
        return blocks + [blank], [blank] + blocks

    def near_product(places):
        rows, even, odd = [], [], []
        for dx, dz in places:
            rows += near_rows(dx, dz)
            first, second = near_weights(dx, dz)
            even += first
            odd += second
        mats = jnp.concatenate(
            [jnp.concatenate(even, axis=1), jnp.concatenate(odd, axis=1)], axis=0
        )
        return dot(jnp.concatenate(rows, axis=1), mats, NT)

    coarse_w[...] = jnp.zeros(coarse_w.shape, BF16)
    ch["last"][0].wait()
    near_acc[...] = near_product([(0, 0)])

    got_first(ch)
    got_first(on)
    got_first(mo)
    tw[0].wait()
    tw[1].start()
    local[8].wait()
    chunk = 8

    def build_coarse(u, carry):
        for t in range(chunk):
            for k in range(2):
                r = 2 * (chunk * u + t) + k
                x, y, z = r // (sizes[1] * sizes[2]), r // sizes[2] % sizes[1], r % sizes[2]
                value = coarse_raw[x, y, z]
                for s in range(2):
                    col = k * pts + s * lane
                    coarse_w[chunk * u + t, s * lane : s * lane + rank, col : col + rank] = value
        return carry

    lax.fori_loop(0, cells // 2 // chunk, build_coarse, 0)

    got_second(on)
    ch["last"][1].wait()
    near_acc[...] += near_product([(-1, 0), (1, 0)])
    tw[1].wait()
    tw[2].start()
    got_second(mo)
    got_edge(on)
    got_second(ch)
    got_edge(mo)
    got_edge(ch)
    tw[2].wait()

    group = 16

    def coarse_step(u, total):
        rows, mats = [], []
        for k in range(group):
            t = u * group + k
            for r in (2 * t, 2 * t + 1):
                x, y, z = r // (sizes[1] * sizes[2]), r // sizes[2] % sizes[1], r % sizes[2]
                rows.append(
                    two[
                        lax.rem(me[0] + x, sizes[0]),
                        lax.rem(me[1] + y, sizes[1]),
                        lax.rem(me[2] + z, sizes[2]),
                    ]
                )
            mats.append(coarse_w[t])
        return total + dot(jnp.concatenate(rows, axis=1), jnp.concatenate(mats, axis=1), NT)

    local_two = lax.fori_loop(
        0, cells // 2 // group, coarse_step, jnp.zeros((half, pts), F32)
    )

    on["last"][0].wait()

    def expand(ref, places):
        n = ref.shape[4]
        tiles = [
            jnp.concatenate(
                [ref[a, q // 2, b, q % 2].reshape(n * half, pts) for a, b in places], axis=0
            )
            for q in range(parts)
        ]
        whole = unpack(tiles)
        for k, (a, b) in enumerate(places):
            piece = whole[k * n * half : (k + 1) * n * half]
            ref[a, 1, b, 1] = piece.reshape(n, half, pts)

    expand(one, [(a, b) for a in range(one.shape[0]) for b in range(one.shape[2])])

    def boxes_of(ref):
        xs, px, ys, py, zs = ref.shape[:5]
        return ref.reshape(xs * px, ys * py, zs, half, pts)

    mom_box, one_box = boxes_of(mom), boxes_of(one)

    def far_window(ref, level, e, count):
        ox, oy, oz = (far_offsets[d, level, e] + 2 for d in range(3))
        planes = []
        for i in range(count[0]):
            x = lax.rem(ox + i, ref.shape[0]) if wrap(ref, count) else ox + i
            v = ref[x, pl.ds(oy, count[1]), pl.ds(oz, count[2])]
            planes.append(v.reshape(count[1] * count[2] * half, pts))
        return jnp.concatenate(planes, axis=0)

    def wrap(ref, count):
        return ref.shape[0] < count[0] + 4

    def far_product(ref, level, t, many, count):
        rows = [far_window(ref, level, 4 * t + k, count) for k in range(4 * many)]
        mats = [far_w[level, t + k] for k in range(many)]
        return dot(jnp.concatenate(rows, axis=1), jnp.concatenate(mats, axis=1), NT)

    one_acc[...] = jnp.zeros(one_acc.shape, F32)

    def far_one(t, carry):
        one_acc[...] += far_product(one_box, 1, 4 * t, 4, (hx, hy, hz))
        return carry

    lax.fori_loop(0, steps // 16, far_one, 0)

    rounded = local_two.astype(BF16)
    for number in range(8):
        rows = slice(number * half, (number + 1) * half)
        one_acc[rows, :] += dot(rounded, trans_w[number], NN)

    rounded = one_acc[...].astype(BF16)
    for number, (i, j, l) in enumerate(kids):
        value = dot(rounded, trans_w[number], NN)
        for n, (a, b, c) in enumerate(parents):
            box = ((2 * a + i) * by + 2 * b + j) * bz + 2 * c + l
            far_acc[box * half : (box + 1) * half, :] = value[n * half : (n + 1) * half]

    ch["last"][2].wait()
    near_acc[...] += near_product([(0, -1), (0, 1)])

    def expand_middle(u, carry):
        expand(mom, [(2 * u + i, b) for i in range(2) for b in range(1, 1 + hy)])
        return carry

    lax.fori_loop(0, mom.shape[0] // 2, expand_middle, 0)
    mo["last"][0].wait()

    def expand_outer(u, carry):
        expand(mom, [(2 * u + i, b) for i in range(2) for b in (0, 1 + hy)])
        return carry

    lax.fori_loop(0, mom.shape[0] // 2, expand_outer, 0)

    def far_zero(t, carry):
        far_acc[...] += far_product(mom_box, 0, 2 * t, 2, (bx, by, bz))
        return carry

    lax.fori_loop(0, steps // 8, far_zero, 0)

    ch["last"][3].wait()
    near_acc[...] += near_product([(-1, -1), (-1, 1)])
    near_acc[...] += near_product([(1, -1), (1, 1)])

    def finish(x, carry):
        span = by * bz * half
        rows = far_acc[pl.ds(pl.multiple_of(x * span, span), span), :].astype(BF16)
        value = dot(rows, basis_w[...], NN)
        for b in range(by * bz):
            y, z = b // bz, b % bz
            live = (lanes < counts[x, y, z]).astype(F32)
            live = jnp.concatenate([live, live], axis=0)
            far = jnp.concatenate(
                [
                    value[b * half : (b + 1) * half, 0:pts],
                    value[b * half : (b + 1) * half, pts : 2 * pts],
                ],
                axis=0,
            )
            at = pl.multiple_of(((y // 2 * bx + x) * bz + z) * rhs, rhs)
            col = y % 2 * pts
            out[x, y, z] = (near_acc[pl.ds(at, rhs), col : col + pts] + far) * live
        return carry

    lax.fori_loop(0, bx, finish, 0)

    drain(send_sem.at[0], sent[0])


def body(
    sizes,
    charges,
    counts,
    near_offsets,
    near_blocks,
    leaf_basis,
    transfer,
    far_offsets,
    coupling,
    coarse_coupling,
):
    bx, by, bz, rhs, pts = charges.shape
    half = rhs // 2
    stencil = near_offsets.shape[0]
    boxes = bx * by * bz
    hx, hy, hz = bx // 2, by // 2, bz // 2
    one_x = hx + 2 if sizes[0] * hx == hx + 2 else hx + 4
    levels, steps = coupling.shape[:2]
    rank = leaf_basis.shape[0]
    parts = rank // (pts // 2 - rank)
    cells = sizes[0] * sizes[1] * sizes[2]
    vmem = pl.BlockSpec(memory_space=pltpu.VMEM)
    hbm = pl.BlockSpec(memory_space=pl.ANY)
    return pl.pallas_call(
        functools.partial(kernel, sizes),
        out_shape=pltpu.VMEM(charges.shape, F32),
        in_specs=[hbm] * 9,
        out_specs=vmem,
        scratch_shapes=[
            pltpu.SMEM((3, stencil), jnp.int32),
            pltpu.SMEM(counts.shape, jnp.int32),
            pltpu.SMEM((3,) + far_offsets.shape[:2], jnp.int32),
            pltpu.VMEM(charges.shape, BF16),
            pltpu.VMEM(leaf_basis.shape, BF16),
            pltpu.VMEM(transfer.shape, BF16),
            pltpu.VMEM((bx + 2, by + 2, bz + 2, rhs, pts), BF16),
            pltpu.VMEM((hx + 2, 2, hy + 2, 2, bz + 4, half, pts), BF16),
            pltpu.VMEM((one_x // 2, 2, hy // 2 + 2, 2, hz + 4, half, pts), BF16),
            pltpu.VMEM(tuple(sizes) + (half, pts), BF16),
            pltpu.VMEM(near_blocks.shape, BF16),
            pltpu.VMEM(coupling.shape, BF16),
            pltpu.VMEM(coarse_coupling.shape, BF16),
            pltpu.VMEM((levels, steps // 4, pts, 4 * pts), BF16),
            pltpu.VMEM((cells // 2, pts, 2 * pts), BF16),
            pltpu.VMEM((8, pts, pts), BF16),
            pltpu.VMEM((pts, 2 * pts), BF16),
            pltpu.VMEM((pts, parts * pts), BF16),
            pltpu.VMEM((boxes // 2 * rhs, 2 * pts), F32),
            pltpu.VMEM((boxes * half, pts), F32),
            pltpu.VMEM((hx * hy * hz * half, pts), F32),
            pltpu.VMEM((512, half, pts), BF16),
            pltpu.SMEM((9,), jnp.int32),
            pltpu.SemaphoreType.DMA((9,)),
            pltpu.SemaphoreType.DMA((1,)),
            pltpu.SemaphoreType.DMA((24,)),
        ],
        compiler_params=pltpu.CompilerParams(
            collective_id=0, has_side_effects=True, vmem_limit_bytes=56 * 1024 * 1024
        ),
    )(
        near_offsets.T,
        counts,
        far_offsets.transpose(2, 0, 1),
        charges,
        leaf_basis,
        transfer,
        near_blocks,
        coupling,
        coarse_coupling,
    )


def solution(mesh):
    sizes = tuple(mesh.shape[a] for a in AXES)
    in_specs = (
        P("gx", "gy", "gz", None, None),
        P("gx", "gy", "gz"),
        P(),
        P(),
        P(),
        P(),
        P(),
        P(),
        P(),
    )
    out_specs = P("gx", "gy", "gz", None, None)
    return jax.shard_map(
        functools.partial(body, sizes),
        mesh=mesh,
        in_specs=in_specs,
        out_specs=out_specs,
        check_vma=False,
    )
```

```python
import functools

import jax
import jax.numpy as jnp
from jax import lax
from jax.experimental import pallas as pl
from jax.experimental.pallas import tpu as pltpu
from jax.sharding import PartitionSpec as P

MESH = pl.DeviceIdType.MESH
AXES = ("gx", "gy", "gz")
F32 = jnp.float32
BF16 = jnp.bfloat16
NT = (((1,), (1,)), ((), ()))
NN = (((1,), (0,)), ((), ()))


def dot(a, b, dims):
    return lax.dot_general(a, b, dims, preferred_element_type=F32)


def kernel(
    sizes,
    near_offsets_hbm,
    counts_hbm,
    far_offsets_hbm,
    charges_hbm,
    basis_hbm,
    transfer_hbm,
    near_hbm,
    coupling_hbm,
    coarse_hbm,
    out,
    near_offsets,
    counts,
    far_offsets,
    charges,
    basis,
    transfer,
    ext,
    mom,
    one,
    two,
    near_w,
    coupling_raw,
    coarse_raw,
    far_w,
    coarse_w,
    trans_w,
    basis_w,
    spread,
    near_acc,
    far_acc,
    one_acc,
    span,
    inverse,
    local_sem,
    send_sem,
    recv_sem,
):
    bx, by, bz, rhs, pts = charges.shape
    rank = basis.shape[0]
    half = rhs // 2
    lane = pts // 2
    me = [lax.axis_index(a) for a in AXES]
    steps = coupling_raw.shape[1]
    cells = sizes[0] * sizes[1] * sizes[2]
    hx, hy, hz = bx // 2, by // 2, bz // 2

    pairs = (
        (counts_hbm, counts),
        (charges_hbm, charges),
        (basis_hbm, basis),
        (transfer_hbm, transfer),
        (near_offsets_hbm, near_offsets),
        (far_offsets_hbm, far_offsets),
        (near_hbm, near_w),
        (coupling_hbm, coupling_raw),
        (coarse_hbm, coarse_raw),
    )
    local = [
        pltpu.make_async_copy(src, dst, local_sem.at[n]) for n, (src, dst) in enumerate(pairs)
    ]
    for copy in local:
        copy.start()

    barrier = pltpu.get_barrier_semaphore()
    peers = 0
    for axis in range(3):
        for d in range(1, sizes[axis]):
            other = lax.rem(me[axis] + d, sizes[axis])
            pl.semaphore_signal(barrier, inc=1, device_id={AXES[axis]: other}, device_id_type=MESH)
            peers += 1

    slots = [0]
    sent = [0]

    def tiles_of(ref):
        count = 1
        for n in ref.shape:
            count *= n
        return count // (half * pts)

    class Batch:
        def __init__(self):
            self.sem = recv_sem.at[slots[0]]
            slots[0] += 1
            self.copies = []
            self.tiles = 0

        def add(self, src, dst, device):
            self.copies.append(
                pltpu.make_async_remote_copy(
                    src_ref=src,
                    dst_ref=dst,
                    send_sem=send_sem.at[0],
                    recv_sem=self.sem,
                    device_id=device,
                    device_id_type=MESH,
                )
            )
            self.tiles += tiles_of(dst)

        def start(self, only=None):
            for c in self.copies if only is None else self.copies[only]:
                c.start()
            if only is None:
                sent[0] += self.tiles

        def wait(self):
            drain(self.sem, self.tiles)

    def drain(sem, tiles):
        while tiles > 0:
            n = min(tiles, span.shape[0])
            view = span.at[pl.ds(0, n)]
            pltpu.make_async_copy(view, view, sem).wait()
            tiles -= n

    def halo(ref, own, width, order, packed):
        extent = [ref.shape[d] for d in ((0, 2, 4) if packed else (0, 1, 2))]
        high = [extent[d] == own[d] + 2 * width[d] for d in range(3)]
        sides = ["lh" if high[d] else "l" for d in range(3)]
        part = {
            "o": lambda d: pl.ds(width[d], own[d]),
            "l": lambda d: pl.ds(0, width[d]),
            "h": lambda d: pl.ds(width[d] + own[d], width[d]),
        }
        first, second, third = order

        def moves(batch, axis, fixed, only="lh"):
            def views(start):
                index = [part[fixed.get(d, "o")](d) for d in range(3)]
                index[axis] = pl.ds(start, w)
                if not packed:
                    return [ref.at[tuple(index)]]
                return [
                    ref.at[index[0], i, index[1], pl.ds(0, 2 - i), index[2]] for i in range(2)
                ]

            n, w = own[axis], width[axis]
            if "l" in only:
                target = {AXES[axis]: lax.rem(me[axis] + 1, sizes[axis])}
                for src, dst in zip(views(n), views(0)):
                    batch.add(src, dst, target)
            if "h" in only and high[axis]:
                target = {AXES[axis]: lax.rem(me[axis] + sizes[axis] - 1, sizes[axis])}
                for src, dst in zip(views(w), views(w + n)):
                    batch.add(src, dst, target)
            return batch

        groups = {"A": [moves(Batch(), first, {}, side) for side in sides[first]]}
        groups["B"] = moves(Batch(), second, {})
        groups["AB"] = [moves(Batch(), second, {first: a}) for a in sides[first]]
        last = [Batch() for k in range(1 if packed else 4)]
        cuts = []
        for k, places in enumerate(
            (
                [{}],
                [{first: a} for a in sides[first]],
                [{second: b} for b in sides[second]],
                [{first: a, second: b} for a in sides[first] for b in sides[second]],
            )
        ):
            batch = last[0] if packed else last[k]
            begin = len(batch.copies)
            for fixed in places:
                moves(batch, third, fixed)
            cuts.append((batch, begin, len(batch.copies)))
        groups["last"] = last
        for batch in last:
            sent[0] += batch.tiles

        def send(k, low=0, high=None):
            batch, begin, end = cuts[k]
            n = end - begin
            high = n if high is None else high
            batch.start(slice(begin + low, begin + high))

        groups["send"] = send
        groups["per"] = len(cuts[0][0].copies[: cuts[0][2]])
        groups["unit"] = 2 if packed else 1
        return groups

    def got_first(groups, k):
        groups["A"][k].wait()
        per = groups["per"]
        groups["AB"][k].start()
        groups["send"](1, k * per, (k + 1) * per)

    def got_second(groups):
        groups["B"].wait()
        groups["send"](2)

    def got_edge(groups, k):
        groups["AB"][k].wait()
        per = groups["per"] * (len(groups["B"].copies) // groups["unit"])
        groups["send"](3, k * per, (k + 1) * per)

    ring = (2, 1, 0)

    def gather(stage):
        axis = ring[stage]
        done = ring[:stage]
        batch = Batch()

        index = [pl.ds(0, sizes[d]) if d in done else pl.ds(me[d], 1) for d in range(3)]
        view = two.at[tuple(index)]
        for d in range(1, sizes[axis]):
            batch.add(view, view, {AXES[axis]: lax.rem(me[axis] + d, sizes[axis])})
        return batch

    parts = spread.shape[1] // pts
    third = rank // parts
    ch = halo(ext, (bx, by, bz), (1, 1, 1), (0, 2, 1), False)
    mo = halo(mom, (hx, hy, bz), (1, 1, 2), (2, 0, 1), True)
    on = halo(one, (hx // 2, hy // 2, hz), (1, 1, 2), (2, 0, 1), True)
    tw = [gather(k) for k in range(3)]

    lanes = lax.broadcasted_iota(jnp.int32, (half, pts), 1)
    local[0].wait()
    local[1].wait()

    def mask_row(b, carry):
        x, y = b // by, b % by
        for z in range(bz):
            live = (lanes < counts[x, y, z]).astype(F32).astype(BF16)
            live = jnp.concatenate([live, live], axis=0)
            ext[1 + x, 1 + y, 1 + z] = charges[x, y, z] * live
        return carry

    lax.fori_loop(0, bx * by, mask_row, 0)
    pl.semaphore_wait(barrier, peers)
    for batch in ch["A"]:
        batch.start()
    ch["send"](0)

    local[2].wait()
    basis_w[...] = jnp.zeros(basis_w.shape, BF16)
    basis_w[0:rank, 0:pts] = basis[...]
    basis_w[lane : lane + rank, pts : 2 * pts] = basis[...]
    target = lax.broadcasted_iota(jnp.int32, (pts, pts), 0)
    source = lax.broadcasted_iota(jnp.int32, (pts, pts), 1)
    moved = jnp.where(source % lane >= rank, source - rank, -pts)
    for q in range(parts):
        hit = (target == moved + q * third).astype(F32).astype(BF16)
        spread[:, q * pts : (q + 1) * pts] = hit

    def pack(last):
        return dot(last, spread[...], NN).astype(BF16)

    def unpack(tiles):
        return dot(jnp.concatenate(tiles, axis=1), spread[...], NT).astype(BF16)

    values = []
    for x in range(bx):
        low = ext[1 + x, 1 : 1 + by, 1 : 1 + bz, 0:half].reshape(by * bz * half, pts)
        high = ext[1 + x, 1 : 1 + by, 1 : 1 + bz, half:rhs].reshape(by * bz * half, pts)
        value = dot(jnp.concatenate([low, high], axis=1), basis_w[...], NT).astype(BF16)
        values.append(value.reshape(hy, 2, bz * half, pts))
    for a in range(hx):
        for b in range(hy):
            tiles = [values[2 * a + q // 2][b, q % 2] for q in range(parts + 1)]
            extra = pack(tiles[parts])
            for q in range(parts + 1):
                tile = tiles[q]
                if q < parts:
                    tile = tile + extra[:, q * pts : (q + 1) * pts]
                mom[1 + a, q // 2, 1 + b, q % 2, 2 : 2 + bz] = tile.reshape(bz, half, pts)
    for batch in mo["A"]:
        batch.start()
    mo["send"](0)

    local[3].wait()
    trans_w[...] = jnp.zeros(trans_w.shape, BF16)
    for c in range(8):
        trans_w[c, 0:rank, 0:rank] = transfer[c]
        trans_w[c, lane : lane + rank, lane : lane + rank] = transfer[c]
    parents = [(a, b, c) for a in range(hx) for b in range(hy) for c in range(hz)]
    kids = [(i, j, l) for i in range(2) for j in range(2) for l in range(2)]
    total = jnp.zeros((len(parents) * half, pts), F32)
    for number, (i, j, l) in enumerate(kids):
        rows = jnp.concatenate(
            [mom[1 + a, i, 1 + b, j, 2 + 2 * c + l] for a, b, c in parents], axis=0
        )
        total = total + dot(rows, trans_w[number], NT)
    value = total.astype(BF16)
    pieces = {p: value[n * half : (n + 1) * half] for n, p in enumerate(parents)}
    for a in range(hx // 2):
        for b in range(hy // 2):
            tiles = [
                jnp.concatenate([pieces[2 * a + i, 2 * b + j, c] for c in range(hz)], axis=0)
                for i in range(2)
                for j in range(2)
            ]
            extra = pack(tiles[parts])
            for q in range(parts + 1):
                tile = tiles[q]
                if q < parts:
                    tile = tile + extra[:, q * pts : (q + 1) * pts]
                one[1 + a, q // 2, 1 + b, q % 2, 2 : 2 + hz] = tile.reshape(hz, half, pts)
    total = jnp.zeros((half, pts), F32)
    for number in range(8):
        total = total + dot(value[number * half : (number + 1) * half], trans_w[number], NT)
    two[me[0], me[1], me[2]] = total.astype(BF16)
    tw[0].start()
    for batch in on["A"]:
        batch.start()
    on["B"].start()
    on["send"](0)

    far_w[...] = jnp.zeros(far_w.shape, BF16)
    coarse_w[...] = jnp.zeros(coarse_w.shape, BF16)
    local[4].wait()
    local[5].wait()
    stencil = near_offsets.shape[1]
    words = [jnp.int32(0)] * 9
    for number in range(stencil):
        x, y, z = (near_offsets[d, number] + 1 for d in range(3))
        key = x * 3 + y
        value = jnp.where(z == 0, number, jnp.where(z == 1, number * 32, number * 1024))
        words = [w + jnp.where(key == k, value, 0) for k, w in enumerate(words)]
    for k in range(9):
        inverse[k] = words[k]
    local[7].wait()

    def build_far(t, carry):
        for level in range(2):
            for u in range(2):
                for k in range(4):
                    value = coupling_raw[level, 8 * t + 4 * u + k]
                    for s in range(2):
                        col = k * pts + s * lane
                        far_w[level, 2 * t + u, s * lane : s * lane + rank, col : col + rank] = value
        return carry

    lax.fori_loop(0, steps // 8, build_far, 0)

    blank = jnp.zeros((pts, pts), BF16)
    pairs_y = by // 2
    half_rows = bx * bz * rhs

    def near_rows(places, j, ks):
        return jnp.concatenate(
            [
                ext[pl.ds(1 + dx, bx), 2 * j + k, pl.ds(1 + dz, bz)].reshape(half_rows, pts)
                for dx, dz in places
                for k in ks
            ],
            axis=1,
        )

    def near_weights(places, ks, lag):
        blocks = []
        for dx, dz in places:
            for k in ks:
                if not 0 <= k - lag < 3:
                    blocks.append(blank)
                    continue
                found = (inverse[(dx + 1) * 3 + k - lag] // 32 ** (dz + 1)) % 32
                blocks.append(near_w[jnp.minimum(found, near_w.shape[0] - 1)])
        return jnp.concatenate(blocks, axis=1)

    def near_own(places, first=False):
        for j in range(pairs_y):
            ks = [k for k in range(4) if 0 <= 2 * j + k - 1 < by]
            mats = jnp.concatenate([near_weights(places, ks, lag) for lag in range(2)], axis=0)
            value = dot(near_rows(places, j, ks), mats, NT)
            at = slice(j * half_rows, (j + 1) * half_rows)
            near_acc[at, :] = value if first else near_acc[at, :] + value

    def near_halo(places):
        for j, k, lag in ((0, 0, 0), (pairs_y - 1, 3, 1)):
            value = dot(near_rows(places, j, [k]), near_weights(places, [k], lag), NT)
            at = slice(j * half_rows, (j + 1) * half_rows)
            near_acc[at, lag * pts : (lag + 1) * pts] += value

    local[6].wait()
    near_own([(0, 0)], True)

    def expand(ref, places):
        n = ref.shape[4]
        tiles = [
            jnp.concatenate(
                [ref[a, q // 2, b, q % 2].reshape(n * half, pts) for a, b in places], axis=0
            )
            for q in range(parts)
        ]
        whole = unpack(tiles)
        for k, (a, b) in enumerate(places):
            piece = whole[k * n * half : (k + 1) * n * half]
            ref[a, 1, b, 1] = piece.reshape(n, half, pts)

    ch["B"].start()
    local[8].wait()
    chunk = 8

    def build_coarse(u, carry):
        for t in range(chunk):
            for k in range(2):
                r = 2 * (chunk * u + t) + k
                x, y, z = r // (sizes[1] * sizes[2]), r // sizes[2] % sizes[1], r % sizes[2]
                value = coarse_raw[x, y, z]
                for s in range(2):
                    col = k * pts + s * lane
                    coarse_w[chunk * u + t, s * lane : s * lane + rank, col : col + rank] = value
        return carry

    lax.fori_loop(0, cells // 2 // chunk, build_coarse, 0)

    got_first(ch, 0)
    mo["B"].start()
    got_first(ch, 1)
    near_own([(-1, 0), (1, 0)])
    tw[0].wait()
    tw[1].start()
    got_first(on, 0)
    got_first(on, 1)
    got_second(on)
    got_first(mo, 0)
    got_first(mo, 1)
    ch["last"][0].wait()
    ch["last"][1].wait()
    near_halo([(0, 0), (-1, 0), (1, 0)])
    tw[1].wait()
    tw[2].start()
    got_second(mo)
    got_second(ch)
    near_own([(0, -1), (0, 1)])
    got_edge(mo, 0)
    got_edge(on, 0)
    got_edge(on, 1)
    got_edge(ch, 0)
    got_edge(ch, 1)
    near_own([(-1, -1), (-1, 1)])
    got_edge(mo, 1)
    near_own([(1, -1), (1, 1)])
    def expand_middle(u, carry):
        expand(mom, [(2 * u + i, b) for i in range(2) for b in range(1, 1 + hy)])
        return carry

    lax.fori_loop(0, mom.shape[0] // 2, expand_middle, 0)
    tw[2].wait()

    group = 16

    def coarse_step(u, total):
        rows, mats = [], []
        for k in range(group):
            t = u * group + k
            for r in (2 * t, 2 * t + 1):
                x, y, z = r // (sizes[1] * sizes[2]), r // sizes[2] % sizes[1], r % sizes[2]
                rows.append(
                    two[
                        lax.rem(me[0] + x, sizes[0]),
                        lax.rem(me[1] + y, sizes[1]),
                        lax.rem(me[2] + z, sizes[2]),
                    ]
                )
            mats.append(coarse_w[t])
        return total + dot(jnp.concatenate(rows, axis=1), jnp.concatenate(mats, axis=1), NT)

    local_two = lax.fori_loop(
        0, cells // 2 // group, coarse_step, jnp.zeros((half, pts), F32)
    )

    on["last"][0].wait()
    expand(one, [(a, b) for a in range(one.shape[0]) for b in range(one.shape[2])])

    def boxes_of(ref):
        xs, px, ys, py, zs = ref.shape[:5]
        return ref.reshape(xs * px, ys * py, zs, half, pts)

    mom_box, one_box = boxes_of(mom), boxes_of(one)

    def far_window(ref, level, e, count):
        ox, oy, oz = (far_offsets[d, level, e] + 2 for d in range(3))
        planes = []
        for i in range(count[0]):
            x = lax.rem(ox + i, ref.shape[0]) if wrap(ref, count) else ox + i
            v = ref[x, pl.ds(oy, count[1]), pl.ds(oz, count[2])]
            planes.append(v.reshape(count[1] * count[2] * half, pts))
        return jnp.concatenate(planes, axis=0)

    def wrap(ref, count):
        return ref.shape[0] < count[0] + 4

    def far_product(ref, level, t, many, count):
        rows = [far_window(ref, level, 4 * t + k, count) for k in range(4 * many)]
        mats = [far_w[level, t + k] for k in range(many)]
        return dot(jnp.concatenate(rows, axis=1), jnp.concatenate(mats, axis=1), NT)

    one_acc[...] = jnp.zeros(one_acc.shape, F32)

    def far_one(t, carry):
        one_acc[...] += far_product(one_box, 1, 4 * t, 4, (hx, hy, hz))
        return carry

    lax.fori_loop(0, steps // 16, far_one, 0)

    rounded = local_two.astype(BF16)
    for number in range(8):
        rows = slice(number * half, (number + 1) * half)
        one_acc[rows, :] += dot(rounded, trans_w[number], NN)

    rounded = one_acc[...].astype(BF16)
    for number, (i, j, l) in enumerate(kids):
        value = dot(rounded, trans_w[number], NN)
        for n, (a, b, c) in enumerate(parents):
            box = ((2 * a + i) * by + 2 * b + j) * bz + 2 * c + l
            far_acc[box * half : (box + 1) * half, :] = value[n * half : (n + 1) * half]

    mo["last"][0].wait()

    expand(mom, [(a, b) for a in range(mom.shape[0]) for b in (0, 1 + hy)])

    def far_zero(t, carry):
        far_acc[...] += far_product(mom_box, 0, 4 * t, 4, (bx, by, bz))
        return carry

    lax.fori_loop(0, steps // 16, far_zero, 0)

    ch["last"][3].wait()
    ch["last"][2].wait()
    near_halo([(dx, dz) for dz in (-1, 1) for dx in (0, -1, 1)])

    def finish(x, carry):
        span = by * bz * half
        rows = far_acc[pl.ds(pl.multiple_of(x * span, span), span), :].astype(BF16)
        value = dot(rows, basis_w[...], NN)
        for b in range(by * bz):
            y, z = b // bz, b % bz
            live = (lanes < counts[x, y, z]).astype(F32)
            live = jnp.concatenate([live, live], axis=0)
            far = jnp.concatenate(
                [
                    value[b * half : (b + 1) * half, 0:pts],
                    value[b * half : (b + 1) * half, pts : 2 * pts],
                ],
                axis=0,
            )
            at = pl.multiple_of(((y // 2 * bx + x) * bz + z) * rhs, rhs)
            col = y % 2 * pts
            out[x, y, z] = (near_acc[pl.ds(at, rhs), col : col + pts] + far) * live
        return carry

    lax.fori_loop(0, bx, finish, 0)

    drain(send_sem.at[0], sent[0])


def body(
    sizes,
    charges,
    counts,
    near_offsets,
    near_blocks,
    leaf_basis,
    transfer,
    far_offsets,
    coupling,
    coarse_coupling,
):
    bx, by, bz, rhs, pts = charges.shape
    half = rhs // 2
    stencil = near_offsets.shape[0]
    boxes = bx * by * bz
    hx, hy, hz = bx // 2, by // 2, bz // 2
    one_x = hx + 2 if sizes[0] * hx == hx + 2 else hx + 4
    levels, steps = coupling.shape[:2]
    rank = leaf_basis.shape[0]
    parts = rank // (pts // 2 - rank)
    cells = sizes[0] * sizes[1] * sizes[2]
    vmem = pl.BlockSpec(memory_space=pltpu.VMEM)
    hbm = pl.BlockSpec(memory_space=pl.ANY)
    return pl.pallas_call(
        functools.partial(kernel, sizes),
        out_shape=pltpu.VMEM(charges.shape, F32),
        in_specs=[hbm] * 9,
        out_specs=vmem,
        scratch_shapes=[
            pltpu.SMEM((3, stencil), jnp.int32),
            pltpu.SMEM(counts.shape, jnp.int32),
            pltpu.SMEM((3,) + far_offsets.shape[:2], jnp.int32),
            pltpu.VMEM(charges.shape, BF16),
            pltpu.VMEM(leaf_basis.shape, BF16),
            pltpu.VMEM(transfer.shape, BF16),
            pltpu.VMEM((bx + 2, by + 2, bz + 2, rhs, pts), BF16),
            pltpu.VMEM((hx + 2, 2, hy + 2, 2, bz + 4, half, pts), BF16),
            pltpu.VMEM((one_x // 2, 2, hy // 2 + 2, 2, hz + 4, half, pts), BF16),
            pltpu.VMEM(tuple(sizes) + (half, pts), BF16),
            pltpu.VMEM(near_blocks.shape, BF16),
            pltpu.VMEM(coupling.shape, BF16),
            pltpu.VMEM(coarse_coupling.shape, BF16),
            pltpu.VMEM((levels, steps // 4, pts, 4 * pts), BF16),
            pltpu.VMEM((cells // 2, pts, 2 * pts), BF16),
            pltpu.VMEM((8, pts, pts), BF16),
            pltpu.VMEM((pts, 2 * pts), BF16),
            pltpu.VMEM((pts, parts * pts), BF16),
            pltpu.VMEM((boxes // 2 * rhs, 2 * pts), F32),
            pltpu.VMEM((boxes * half, pts), F32),
            pltpu.VMEM((hx * hy * hz * half, pts), F32),
            pltpu.VMEM((512, half, pts), BF16),
            pltpu.SMEM((9,), jnp.int32),
            pltpu.SemaphoreType.DMA((9,)),
            pltpu.SemaphoreType.DMA((1,)),
            pltpu.SemaphoreType.DMA((24,)),
        ],
        compiler_params=pltpu.CompilerParams(
            collective_id=0, has_side_effects=True, vmem_limit_bytes=56 * 1024 * 1024
        ),
    )(
        near_offsets.T,
        counts,
        far_offsets.transpose(2, 0, 1),
        charges,
        leaf_basis,
        transfer,
        near_blocks,
        coupling,
        coarse_coupling,
    )


def solution(mesh):
    sizes = tuple(mesh.shape[a] for a in AXES)
    in_specs = (
        P("gx", "gy", "gz", None, None),
        P("gx", "gy", "gz"),
        P(),
        P(),
        P(),
        P(),
        P(),
        P(),
        P(),
    )
    out_specs = P("gx", "gy", "gz", None, None)
    return jax.shard_map(
        functools.partial(body, sizes),
        mesh=mesh,
        in_specs=in_specs,
        out_specs=out_specs,
        check_vma=False,
    )
```

```python
import functools

import jax
import jax.numpy as jnp
from jax import lax
from jax.experimental import pallas as pl
from jax.experimental.pallas import tpu as pltpu
from jax.sharding import PartitionSpec as P

MESH = pl.DeviceIdType.MESH
AXES = ("gx", "gy", "gz")
F32 = jnp.float32
BF16 = jnp.bfloat16
NT = (((1,), (1,)), ((), ()))
NN = (((1,), (0,)), ((), ()))


def dot(a, b, dims):
    return lax.dot_general(a, b, dims, preferred_element_type=F32)


def kernel(
    sizes,
    near_offsets_hbm,
    counts_hbm,
    far_offsets_hbm,
    charges_hbm,
    basis_hbm,
    transfer_hbm,
    near_hbm,
    coupling_hbm,
    coarse_hbm,
    out,
    near_offsets,
    counts,
    far_offsets,
    charges,
    basis,
    transfer,
    ext,
    mom,
    one,
    two,
    near_w,
    coupling_raw,
    coarse_raw,
    far_w,
    coarse_w,
    trans_w,
    basis_w,
    spread,
    near_acc,
    far_acc,
    one_acc,
    span,
    inverse,
    local_sem,
    send_sem,
    recv_sem,
):
    bx, by, bz, rhs, pts = charges.shape
    rank = basis.shape[0]
    half = rhs // 2
    lane = pts // 2
    me = [lax.axis_index(a) for a in AXES]
    steps = coupling_raw.shape[1]
    cells = sizes[0] * sizes[1] * sizes[2]
    hx, hy, hz = bx // 2, by // 2, bz // 2

    pairs = (
        (counts_hbm, counts),
        (charges_hbm, charges),
        (basis_hbm, basis),
        (transfer_hbm, transfer),
        (near_offsets_hbm, near_offsets),
        (far_offsets_hbm, far_offsets),
        (near_hbm, near_w),
        (coupling_hbm, coupling_raw),
        (coarse_hbm, coarse_raw),
    )
    local = [
        pltpu.make_async_copy(src, dst, local_sem.at[n]) for n, (src, dst) in enumerate(pairs)
    ]
    for copy in local:
        copy.start()

    barrier = pltpu.get_barrier_semaphore()
    peers = 0
    for axis in range(3):
        for d in range(1, sizes[axis]):
            other = lax.rem(me[axis] + d, sizes[axis])
            pl.semaphore_signal(barrier, inc=1, device_id={AXES[axis]: other}, device_id_type=MESH)
            peers += 1

    slots = [0]
    sent = [0]

    def tiles_of(ref):
        count = 1
        for n in ref.shape:
            count *= n
        return count // (half * pts)

    class Batch:
        def __init__(self):
            self.sem = recv_sem.at[slots[0]]
            slots[0] += 1
            self.copies = []
            self.tiles = 0

        def add(self, src, dst, device):
            self.copies.append(
                pltpu.make_async_remote_copy(
                    src_ref=src,
                    dst_ref=dst,
                    send_sem=send_sem.at[0],
                    recv_sem=self.sem,
                    device_id=device,
                    device_id_type=MESH,
                )
            )
            self.tiles += tiles_of(dst)

        def start(self, only=None):
            for c in self.copies if only is None else self.copies[only]:
                c.start()
            if only is None:
                sent[0] += self.tiles

        def wait(self):
            drain(self.sem, self.tiles)

    def drain(sem, tiles):
        while tiles > 0:
            n = min(tiles, span.shape[0])
            view = span.at[pl.ds(0, n)]
            pltpu.make_async_copy(view, view, sem).wait()
            tiles -= n

    def halo(ref, own, width, order, packed):
        extent = [ref.shape[d] for d in ((0, 2, 4) if packed else (0, 1, 2))]
        high = [extent[d] == own[d] + 2 * width[d] for d in range(3)]
        sides = ["lh" if high[d] else "l" for d in range(3)]
        part = {
            "o": lambda d: pl.ds(width[d], own[d]),
            "l": lambda d: pl.ds(0, width[d]),
            "h": lambda d: pl.ds(width[d] + own[d], width[d]),
        }
        first, second, third = order

        def moves(batch, axis, fixed, only="lh"):
            def views(start):
                index = [part[fixed.get(d, "o")](d) for d in range(3)]
                index[axis] = pl.ds(start, w)
                if not packed:
                    return [ref.at[tuple(index)]]
                return [
                    ref.at[index[0], i, index[1], pl.ds(0, 2 - i), index[2]] for i in range(2)
                ]

            n, w = own[axis], width[axis]
            if "l" in only:
                target = {AXES[axis]: lax.rem(me[axis] + 1, sizes[axis])}
                for src, dst in zip(views(n), views(0)):
                    batch.add(src, dst, target)
            if "h" in only and high[axis]:
                target = {AXES[axis]: lax.rem(me[axis] + sizes[axis] - 1, sizes[axis])}
                for src, dst in zip(views(w), views(w + n)):
                    batch.add(src, dst, target)
            return batch

        groups = {"A": [moves(Batch(), first, {}, side) for side in sides[first]]}
        groups["B"] = moves(Batch(), second, {})
        groups["AB"] = [
            [moves(Batch(), second, {first: a}, b) for b in sides[second]] for a in sides[first]
        ]
        last = [Batch() for k in range(1 if packed else 4)]
        cuts = []
        for k, places in enumerate(
            (
                [{}],
                [{first: a} for a in sides[first]],
                [{second: b} for b in sides[second]],
                [{first: a, second: b} for a in sides[first] for b in sides[second]],
            )
        ):
            batch = last[0] if packed else last[k]
            begin = len(batch.copies)
            for fixed in places:
                moves(batch, third, fixed)
            cuts.append((batch, begin, len(batch.copies)))
        groups["last"] = last
        for batch in last:
            sent[0] += batch.tiles

        def send(k, low=0, high=None):
            batch, begin, end = cuts[k]
            n = end - begin
            high = n if high is None else high
            batch.start(slice(begin + low, begin + high))

        groups["send"] = send
        groups["per"] = len(cuts[0][0].copies[: cuts[0][2]])
        groups["unit"] = 2 if packed else 1
        return groups

    def got_first(groups, k):
        groups["A"][k].wait()
        per = groups["per"]
        for batch in groups["AB"][k]:
            batch.start()
        groups["send"](1, k * per, (k + 1) * per)

    def got_second(groups):
        groups["B"].wait()
        groups["send"](2)

    def got_edge(groups, k):
        per = groups["per"]
        for n, batch in enumerate(groups["AB"][k]):
            batch.wait()
            n += k * len(groups["AB"][k])
            groups["send"](3, n * per, (n + 1) * per)

    ring = (2, 1, 0)

    def gather(stage):
        axis = ring[stage]
        done = ring[:stage]
        batch = Batch()

        index = [pl.ds(0, sizes[d]) if d in done else pl.ds(me[d], 1) for d in range(3)]
        view = two.at[tuple(index)]
        for d in range(1, sizes[axis]):
            batch.add(view, view, {AXES[axis]: lax.rem(me[axis] + d, sizes[axis])})
        return batch

    parts = spread.shape[1] // pts
    third = rank // parts
    ch = halo(ext, (bx, by, bz), (1, 1, 1), (0, 2, 1), False)
    mo = halo(mom, (hx, hy, bz), (1, 1, 2), (2, 0, 1), True)
    on = halo(one, (hx // 2, hy // 2, hz), (1, 1, 2), (2, 0, 1), True)
    tw = [gather(k) for k in range(3)]

    lanes = lax.broadcasted_iota(jnp.int32, (half, pts), 1)
    local[0].wait()
    local[1].wait()

    def mask_row(b, carry):
        x, y = b // by, b % by
        for z in range(bz):
            live = (lanes < counts[x, y, z]).astype(F32).astype(BF16)
            live = jnp.concatenate([live, live], axis=0)
            ext[1 + x, 1 + y, 1 + z] = charges[x, y, z] * live
        return carry

    lax.fori_loop(0, bx * by, mask_row, 0)
    pl.semaphore_wait(barrier, peers)
    for batch in ch["A"]:
        batch.start()
    ch["send"](0)

    local[2].wait()
    basis_w[...] = jnp.zeros(basis_w.shape, BF16)
    basis_w[0:rank, 0:pts] = basis[...]
    basis_w[lane : lane + rank, pts : 2 * pts] = basis[...]
    target = lax.broadcasted_iota(jnp.int32, (pts, pts), 0)
    source = lax.broadcasted_iota(jnp.int32, (pts, pts), 1)
    moved = jnp.where(source % lane >= rank, source - rank, -pts)
    for q in range(parts):
        hit = (target == moved + q * third).astype(F32).astype(BF16)
        spread[:, q * pts : (q + 1) * pts] = hit

    def pack(last):
        return dot(last, spread[...], NN).astype(BF16)

    def unpack(tiles):
        return dot(jnp.concatenate(tiles, axis=1), spread[...], NT).astype(BF16)

    values = []
    for x in range(bx):
        low = ext[1 + x, 1 : 1 + by, 1 : 1 + bz, 0:half].reshape(by * bz * half, pts)
        high = ext[1 + x, 1 : 1 + by, 1 : 1 + bz, half:rhs].reshape(by * bz * half, pts)
        value = dot(jnp.concatenate([low, high], axis=1), basis_w[...], NT).astype(BF16)
        values.append(value.reshape(hy, 2, bz * half, pts))
    for a in range(hx):
        for b in range(hy):
            tiles = [values[2 * a + q // 2][b, q % 2] for q in range(parts + 1)]
            extra = pack(tiles[parts])
            for q in range(parts + 1):
                tile = tiles[q]
                if q < parts:
                    tile = tile + extra[:, q * pts : (q + 1) * pts]
                mom[1 + a, q // 2, 1 + b, q % 2, 2 : 2 + bz] = tile.reshape(bz, half, pts)
    for batch in mo["A"]:
        batch.start()
    mo["send"](0)

    local[3].wait()
    trans_w[...] = jnp.zeros(trans_w.shape, BF16)
    for c in range(8):
        trans_w[c, 0:rank, 0:rank] = transfer[c]
        trans_w[c, lane : lane + rank, lane : lane + rank] = transfer[c]
    parents = [(a, b, c) for a in range(hx) for b in range(hy) for c in range(hz)]
    kids = [(i, j, l) for i in range(2) for j in range(2) for l in range(2)]
    total = jnp.zeros((len(parents) * half, pts), F32)
    for number, (i, j, l) in enumerate(kids):
        rows = jnp.concatenate(
            [mom[1 + a, i, 1 + b, j, 2 + 2 * c + l] for a, b, c in parents], axis=0
        )
        total = total + dot(rows, trans_w[number], NT)
    value = total.astype(BF16)
    pieces = {p: value[n * half : (n + 1) * half] for n, p in enumerate(parents)}
    for a in range(hx // 2):
        for b in range(hy // 2):
            tiles = [
                jnp.concatenate([pieces[2 * a + i, 2 * b + j, c] for c in range(hz)], axis=0)
                for i in range(2)
                for j in range(2)
            ]
            extra = pack(tiles[parts])
            for q in range(parts + 1):
                tile = tiles[q]
                if q < parts:
                    tile = tile + extra[:, q * pts : (q + 1) * pts]
                one[1 + a, q // 2, 1 + b, q % 2, 2 : 2 + hz] = tile.reshape(hz, half, pts)
    total = jnp.zeros((half, pts), F32)
    for number in range(8):
        total = total + dot(value[number * half : (number + 1) * half], trans_w[number], NT)
    two[me[0], me[1], me[2]] = total.astype(BF16)
    tw[0].start()
    for batch in on["A"]:
        batch.start()
    on["B"].start()
    on["send"](0)

    far_w[...] = jnp.zeros(far_w.shape, BF16)
    coarse_w[...] = jnp.zeros(coarse_w.shape, BF16)
    local[4].wait()
    local[5].wait()
    stencil = near_offsets.shape[1]
    words = [jnp.int32(0)] * 9
    for number in range(stencil):
        x, y, z = (near_offsets[d, number] + 1 for d in range(3))
        key = x * 3 + y
        value = jnp.where(z == 0, number, jnp.where(z == 1, number * 32, number * 1024))
        words = [w + jnp.where(key == k, value, 0) for k, w in enumerate(words)]
    for k in range(9):
        inverse[k] = words[k]
    local[7].wait()

    def build_far(t, carry):
        for level in range(2):
            for u in range(2):
                for k in range(4):
                    value = coupling_raw[level, 8 * t + 4 * u + k]
                    for s in range(2):
                        col = k * pts + s * lane
                        far_w[level, 2 * t + u, s * lane : s * lane + rank, col : col + rank] = value
        return carry

    lax.fori_loop(0, steps // 8, build_far, 0)

    blank = jnp.zeros((pts, pts), BF16)
    pairs_y = by // 2
    half_rows = bx * bz * rhs

    def near_rows(places, j, ks):
        return jnp.concatenate(
            [
                ext[pl.ds(1 + dx, bx), 2 * j + k, pl.ds(1 + dz, bz)].reshape(half_rows, pts)
                for dx, dz in places
                for k in ks
            ],
            axis=1,
        )

    def near_weights(places, ks, lag):
        blocks = []
        for dx, dz in places:
            for k in ks:
                if not 0 <= k - lag < 3:
                    blocks.append(blank)
                    continue
                found = (inverse[(dx + 1) * 3 + k - lag] // 32 ** (dz + 1)) % 32
                blocks.append(near_w[jnp.minimum(found, near_w.shape[0] - 1)])
        return jnp.concatenate(blocks, axis=1)

    def near_own(places, first=False):
        for j in range(pairs_y):
            ks = [k for k in range(4) if 0 <= 2 * j + k - 1 < by]
            mats = jnp.concatenate([near_weights(places, ks, lag) for lag in range(2)], axis=0)
            value = dot(near_rows(places, j, ks), mats, NT)
            at = slice(j * half_rows, (j + 1) * half_rows)
            near_acc[at, :] = value if first else near_acc[at, :] + value

    def near_halo(places):
        for j, k, lag in ((0, 0, 0), (pairs_y - 1, 3, 1)):
            value = dot(near_rows(places, j, [k]), near_weights(places, [k], lag), NT)
            at = slice(j * half_rows, (j + 1) * half_rows)
            near_acc[at, lag * pts : (lag + 1) * pts] += value

    local[6].wait()
    near_own([(0, 0)], True)

    def expand(ref, places):
        n = ref.shape[4]
        tiles = [
            jnp.concatenate(
                [ref[a, q // 2, b, q % 2].reshape(n * half, pts) for a, b in places], axis=0
            )
            for q in range(parts)
        ]
        whole = unpack(tiles)
        for k, (a, b) in enumerate(places):
            piece = whole[k * n * half : (k + 1) * n * half]
            ref[a, 1, b, 1] = piece.reshape(n, half, pts)

    ch["B"].start()
    local[8].wait()
    chunk = 8

    def build_coarse(u, carry):
        for t in range(chunk):
            for k in range(2):
                r = 2 * (chunk * u + t) + k
                x, y, z = r // (sizes[1] * sizes[2]), r // sizes[2] % sizes[1], r % sizes[2]
                value = coarse_raw[x, y, z]
                for s in range(2):
                    col = k * pts + s * lane
                    coarse_w[chunk * u + t, s * lane : s * lane + rank, col : col + rank] = value
        return carry

    lax.fori_loop(0, cells // 2 // chunk, build_coarse, 0)

    got_first(ch, 0)
    mo["B"].start()
    got_first(ch, 1)
    near_own([(-1, 0), (1, 0)])
    tw[0].wait()
    tw[1].start()
    for k in range(len(on["A"])):
        got_first(on, k)
    got_second(on)
    got_first(mo, 0)
    got_first(mo, 1)
    ch["last"][0].wait()
    ch["last"][1].wait()
    near_halo([(0, 0), (-1, 0), (1, 0)])
    tw[1].wait()
    tw[2].start()
    got_second(mo)
    got_second(ch)
    near_own([(0, -1), (0, 1)])
    got_edge(mo, 0)
    for k in range(len(on["A"])):
        got_edge(on, k)
    got_edge(ch, 0)
    got_edge(ch, 1)
    near_own([(-1, -1), (-1, 1)])
    got_edge(mo, 1)

    near_own([(1, -1), (1, 1)])
    def expand_middle(u, carry):
        expand(mom, [(2 * u + i, b) for i in range(2) for b in range(1, 1 + hy)])
        return carry

    lax.fori_loop(0, mom.shape[0] // 2, expand_middle, 0)
    tw[2].wait()

    group = 16

    def coarse_step(u, total):
        rows, mats = [], []
        for k in range(group):
            t = u * group + k
            for r in (2 * t, 2 * t + 1):
                x, y, z = r // (sizes[1] * sizes[2]), r // sizes[2] % sizes[1], r % sizes[2]
                rows.append(
                    two[
                        lax.rem(me[0] + x, sizes[0]),
                        lax.rem(me[1] + y, sizes[1]),
                        lax.rem(me[2] + z, sizes[2]),
                    ]
                )
            mats.append(coarse_w[t])
        return total + dot(jnp.concatenate(rows, axis=1), jnp.concatenate(mats, axis=1), NT)

    local_two = lax.fori_loop(
        0, cells // 2 // group, coarse_step, jnp.zeros((half, pts), F32)
    )

    on["last"][0].wait()
    expand(one, [(a, b) for a in range(one.shape[0]) for b in range(one.shape[2])])

    def boxes_of(ref):
        xs, px, ys, py, zs = ref.shape[:5]
        return ref.reshape(xs * px, ys * py, zs, half, pts)

    mom_box, one_box = boxes_of(mom), boxes_of(one)

    def far_window(ref, level, e, count):
        ox, oy, oz = (far_offsets[d, level, e] + 2 for d in range(3))
        planes = []
        for i in range(count[0]):
            x = lax.rem(ox + i, ref.shape[0]) if wrap(ref, count) else ox + i
            v = ref[x, pl.ds(oy, count[1]), pl.ds(oz, count[2])]
            planes.append(v.reshape(count[1] * count[2] * half, pts))
        return jnp.concatenate(planes, axis=0)

    def wrap(ref, count):
        return ref.shape[0] < count[0] + 4

    def far_product(ref, level, t, many, count):
        rows = [far_window(ref, level, 4 * t + k, count) for k in range(4 * many)]
        mats = [far_w[level, t + k] for k in range(many)]
        return dot(jnp.concatenate(rows, axis=1), jnp.concatenate(mats, axis=1), NT)

    one_acc[...] = jnp.zeros(one_acc.shape, F32)

    def far_one(t, carry):
        one_acc[...] += far_product(one_box, 1, 4 * t, 4, (hx, hy, hz))
        return carry

    lax.fori_loop(0, steps // 16, far_one, 0)

    rounded = local_two.astype(BF16)
    for number in range(8):
        rows = slice(number * half, (number + 1) * half)
        one_acc[rows, :] += dot(rounded, trans_w[number], NN)

    rounded = one_acc[...].astype(BF16)
    for number, (i, j, l) in enumerate(kids):
        value = dot(rounded, trans_w[number], NN)
        for n, (a, b, c) in enumerate(parents):
            box = ((2 * a + i) * by + 2 * b + j) * bz + 2 * c + l
            far_acc[box * half : (box + 1) * half, :] = value[n * half : (n + 1) * half]

    mo["last"][0].wait()

    expand(mom, [(a, b) for a in range(mom.shape[0]) for b in (0, 1 + hy)])

    def far_zero(t, carry):
        far_acc[...] += far_product(mom_box, 0, 4 * t, 4, (bx, by, bz))
        return carry

    lax.fori_loop(0, steps // 16, far_zero, 0)

    ch["last"][3].wait()
    ch["last"][2].wait()
    near_halo([(dx, dz) for dz in (-1, 1) for dx in (0, -1, 1)])

    def finish_plane(x):
        span = by * bz * half
        rows = far_acc[pl.ds(pl.multiple_of(x * span, span), span), :].astype(BF16)
        value = dot(rows, basis_w[...], NN)
        for b in range(by * bz):
            y, z = b // bz, b % bz
            live = (lanes < counts[x, y, z]).astype(F32)
            live = jnp.concatenate([live, live], axis=0)
            far = jnp.concatenate(
                [
                    value[b * half : (b + 1) * half, 0:pts],
                    value[b * half : (b + 1) * half, pts : 2 * pts],
                ],
                axis=0,
            )
            at = pl.multiple_of(((y // 2 * bx + x) * bz + z) * rhs, rhs)
            col = y % 2 * pts
            out[x, y, z] = (near_acc[pl.ds(at, rhs), col : col + pts] + far) * live

    def finish(t, carry):
        for u in range(2):
            finish_plane(2 * t + u)
        return carry

    lax.fori_loop(0, hx, finish, 0)

    drain(send_sem.at[0], sent[0])


def body(
    sizes,
    charges,
    counts,
    near_offsets,
    near_blocks,
    leaf_basis,
    transfer,
    far_offsets,
    coupling,
    coarse_coupling,
):
    bx, by, bz, rhs, pts = charges.shape
    half = rhs // 2
    stencil = near_offsets.shape[0]
    boxes = bx * by * bz
    hx, hy, hz = bx // 2, by // 2, bz // 2
    one_x = hx + 2 if sizes[0] * hx == hx + 2 else hx + 4
    levels, steps = coupling.shape[:2]
    rank = leaf_basis.shape[0]
    parts = rank // (pts // 2 - rank)
    cells = sizes[0] * sizes[1] * sizes[2]
    vmem = pl.BlockSpec(memory_space=pltpu.VMEM)
    hbm = pl.BlockSpec(memory_space=pl.ANY)
    return pl.pallas_call(
        functools.partial(kernel, sizes),
        out_shape=pltpu.VMEM(charges.shape, F32),
        in_specs=[hbm] * 9,
        out_specs=vmem,
        scratch_shapes=[
            pltpu.SMEM((3, stencil), jnp.int32),
            pltpu.SMEM(counts.shape, jnp.int32),
            pltpu.SMEM((3,) + far_offsets.shape[:2], jnp.int32),
            pltpu.VMEM(charges.shape, BF16),
            pltpu.VMEM(leaf_basis.shape, BF16),
            pltpu.VMEM(transfer.shape, BF16),
            pltpu.VMEM((bx + 2, by + 2, bz + 2, rhs, pts), BF16),
            pltpu.VMEM((hx + 2, 2, hy + 2, 2, bz + 4, half, pts), BF16),
            pltpu.VMEM((one_x // 2, 2, hy // 2 + 2, 2, hz + 4, half, pts), BF16),
            pltpu.VMEM(tuple(sizes) + (half, pts), BF16),
            pltpu.VMEM(near_blocks.shape, BF16),
            pltpu.VMEM(coupling.shape, BF16),
            pltpu.VMEM(coarse_coupling.shape, BF16),
            pltpu.VMEM((levels, steps // 4, pts, 4 * pts), BF16),
            pltpu.VMEM((cells // 2, pts, 2 * pts), BF16),
            pltpu.VMEM((8, pts, pts), BF16),
            pltpu.VMEM((pts, 2 * pts), BF16),
            pltpu.VMEM((pts, parts * pts), BF16),
            pltpu.VMEM((boxes // 2 * rhs, 2 * pts), F32),
            pltpu.VMEM((boxes * half, pts), F32),
            pltpu.VMEM((hx * hy * hz * half, pts), F32),
            pltpu.VMEM((512, half, pts), BF16),
            pltpu.SMEM((9,), jnp.int32),
            pltpu.SemaphoreType.DMA((9,)),
            pltpu.SemaphoreType.DMA((1,)),
            pltpu.SemaphoreType.DMA((32,)),
        ],
        compiler_params=pltpu.CompilerParams(
            collective_id=0, has_side_effects=True, vmem_limit_bytes=56 * 1024 * 1024
        ),
    )(
        near_offsets.T,
        counts,
        far_offsets.transpose(2, 0, 1),
        charges,
        leaf_basis,
        transfer,
        near_blocks,
        coupling,
        coarse_coupling,
    )


def solution(mesh):
    sizes = tuple(mesh.shape[a] for a in AXES)
    in_specs = (
        P("gx", "gy", "gz", None, None),
        P("gx", "gy", "gz"),
        P(),
        P(),
        P(),
        P(),
        P(),
        P(),
        P(),
    )
    out_specs = P("gx", "gy", "gz", None, None)
    return jax.shard_map(
        functools.partial(body, sizes),
        mesh=mesh,
        in_specs=in_specs,
        out_specs=out_specs,
        check_vma=False,
    )
```
